32 devices in a mesh: freq: 16 (over z, y, x), slab: 2 (over core).
Axes of the slice: x: 2, y: 2, z: 4, core: 2. Of those that a mesh axis runs over, the one named last changes fastest.
Arguments:
- log_conductivity: float32 [10, 32, 128], P('slab'), may hold values from -1 to 1
- omega: float32 [16], P('freq'), may hold values from 0.1 to 2
- sources: float32 [16, 2, 2, 3, 10, 32, 128], P('freq', None, None, None, 'slab'), may hold values from -8 to 8
- receivers: int32 [256], P('slab'), may hold values from 0 to 20479
- observed: float32 [16, 2, 2, 3, 256], P('freq', None, None, None, 'slab'), may hold values from -2.4 to 2.4
- data_weight: float32 [16, 2, 3, 256], P('freq', None, None, 'slab'), may hold values from 3 to 30
- prior_gradient: float32 [10, 32, 128], P('slab', 'freq'), may hold values from -6 to 6
- prior_direction: float32 [10, 32, 128], P('slab', 'freq'), may hold values from -6 to 6
- step_length: float32 [1], replicated, may hold values from 0.2 to 0.6
Outputs:
- unit_direction: float32 [10, 32, 128], P('slab', 'freq')
- trial_model: float32 [10, 32, 128], P('slab')
The draws below stay inside these ranges and needn't reach their ends.
Inputs may be any that keep to these rules, and one draw needn't show every extreme that they name: Each block of 128 receivers belongs to one slab of 5 layers, slabs in order; an entry is z * 32 * 128 + y * 128 + x within its slab; cells may repeat.
All inputs are finite; a program needn't handle non-finite values.
Results may differ from the reference program's by a relative error of at most 0.0011.
Values sent between devices are 32-bit elements; how exact they have to be, the bound alone decides.
A program may use at most 128 MiB of HBM per device.

```python
import math
import jax
import jax.numpy as jnp
from jax import lax

NX = 128
NY = 32
CZ = 5
REC_DEV = 128
ITERS = 4
FREQS = 16
NZ = 10
RECS = 256


def draw_sources(key, part):
    shape = (FREQS, 2, 2, 3, NZ, NY, NX)
    depth_scale = (0.5 + jnp.arange(NZ, dtype=jnp.float32) / NZ)[:, None, None]
    drawn_values = jax.random.normal(key, shape, jnp.float32) * depth_scale
    return jnp.clip(drawn_values, -8.0, 8.0)


def place_ends(entries, own_key, low, high):
    longest = entries.shape.index(max(entries.shape))
    spots = []
    for shift in (0, 1):
        where = [jax.random.randint(jax.random.fold_in(own_key, axis), (), 0, length) for axis, length in enumerate(entries.shape)]
        where[longest] = (where[longest] + shift) % entries.shape[longest]
        spots.append(tuple(where))
    return entries.at[spots[0]].set(low).at[spots[1]].set(high)


def level_of(key, shape, cuts, smallest, largest):
    level, own = 1.0, jax.random.fold_in(key, 6)
    for position, shards_of in cuts:
        draws = jnp.exp(jax.random.uniform(jax.random.fold_in(own, position), (shards_of,), jnp.float32, smallest / len(cuts), largest / len(cuts)))
        level = level * jnp.repeat(draws, shape[position] // shards_of).reshape([-1 if axis == position else 1 for axis in range(len(shape))])
    return level


def noise(key, shape, scale, most, shards=(), kind=jnp.bfloat16):
    factor_of = level_of(key, shape, shards, -0.22, 0.18) if shards else 1.0
    result = jax.random.normal(key, shape, jnp.float32) * scale * factor_of
    return jnp.minimum(jnp.maximum(result, -most), most).astype(kind)


def setup_inputs(seed: int = 0) -> dict:
    key_of = jax.random.split(jax.random.key(seed), 10)
    log_conductivity = jnp.clip(jax.random.uniform(key_of[0], (NZ, NY, NX), jnp.float32, -1.0, 1.0) * level_of(key_of[0], (NZ, NY, NX), ((0, 2),), -0.4, 0.0), -1.0, 1.0)
    omega = jnp.clip(jnp.exp(math.log(2.0) - 2.9957323 * jax.random.uniform(key_of[1], (FREQS,), jnp.float32) ** level_of(key_of[1], (FREQS,), ((0, 16),), -0.2, 0.2)), 0.1, 2.0)
    sources = draw_sources(jax.random.fold_in(key_of[9], 71), 0)
    receivers = place_ends(jax.random.randint(key_of[3], (RECS,), 0, CZ * NY * NX), jax.random.fold_in(key_of[3], 1), 0, (CZ * NY * NX) - 1).astype(jnp.int32)
    observed = noise(key_of[4], (FREQS, 2, 2, 3, RECS), 0.3, 2.4, ((0, 16), (4, 2)), jnp.float32)
    data_weight = jnp.clip(jnp.exp(math.log(30.0) - 2.3025851 * jax.random.uniform(key_of[5], (FREQS, 2, 3, RECS), jnp.float32) ** level_of(key_of[5], (FREQS, 2, 3, RECS), ((0, 16), (3, 2)), -0.2, 0.2)), 3.0, 30.0)
    prior_gradient = noise(key_of[6], (NZ, NY, NX), 1.0, 6.0, ((0, 2), (1, 16)), jnp.float32)
    prior_direction = noise(key_of[7], (NZ, NY, NX), 1.0, 6.0, ((0, 2), (1, 16)), jnp.float32)
    step_length = jnp.clip(jax.random.uniform(key_of[8], (1,), jnp.float32, 0.2, 0.6), 0.2, 0.6)
    return {"log_conductivity": log_conductivity, "omega": omega, "sources": sources, "receivers": receivers, "observed": observed, "data_weight": data_weight, "prior_gradient": prior_gradient, "prior_direction": prior_direction, "step_length": step_length}


epsilon = 1e-06

def complex_div(dividend, divisor):
    modulus = divisor[0] * divisor[0] + divisor[1] * divisor[1]
    return jnp.stack([(dividend[0] * divisor[0] + dividend[1] * divisor[1]) / modulus, (dividend[1] * divisor[0] - dividend[0] * divisor[1]) / modulus])

def scaled(factor, vector):
    factor_re = factor[0][:, None, None, None, None]
    factor_im = factor[1][:, None, None, None, None]
    return jnp.stack([factor_re * vector[:, 0] - factor_im * vector[:, 1], factor_re * vector[:, 1] + factor_im * vector[:, 0]], axis=1)

def inner_sums(former, latter):
    real_part = lax.optimization_barrier(jnp.sum(former[:, 0] * latter[:, 0] - former[:, 1] * latter[:, 1], axis=(1, 2, 3, 4)))
    imag_part = lax.optimization_barrier(jnp.sum(former[:, 0] * latter[:, 1] + former[:, 1] * latter[:, 0], axis=(1, 2, 3, 4)))
    return jnp.stack([real_part, imag_part])

def operate(electric, coupling):
    padded = jnp.pad(electric, ((0, 0), (0, 0), (0, 0), (1, 1), (1, 1), (1, 1)))
    beside = padded[..., 2:, 1:-1, 1:-1] + padded[..., :-2, 1:-1, 1:-1]
    beside = beside + padded[..., 1:-1, 2:, 1:-1] + padded[..., 1:-1, :-2, 1:-1]
    beside = beside + padded[..., 1:-1, 1:-1, 2:] + padded[..., 1:-1, 1:-1, :-2]
    laplace = 6.0 * electric - beside
    return jnp.stack([laplace[:, 0] - coupling * electric[:, 1], laplace[:, 1] + coupling * electric[:, 0]], axis=1)

def krylov_solve(source, coupling):
    solution = jnp.zeros_like(source)
    residual = source
    direction = source
    rho_now = inner_sums(residual, residual)
    for iteration in range(ITERS):
        image = operate(direction, coupling)
        alpha_step = complex_div(rho_now, inner_sums(direction, image))
        solution = solution + scaled(alpha_step, direction)
        residual = residual - scaled(alpha_step, image)
        if iteration + 1 < ITERS:
            rho_next = inner_sums(residual, residual)
            beta_ratio = complex_div(rho_next, rho_now)
            direction = residual + scaled(beta_ratio, direction)
            rho_now = rho_next
    return solution

def reference(log_conductivity, omega, sources, receivers, observed, data_weight, prior_gradient, prior_direction, step_length):
    conductivity = jnp.exp(log_conductivity)
    slab_cells = CZ * NY * NX
    owner_slab = jnp.arange(RECS, dtype=jnp.int32) // REC_DEV
    flat_index = (owner_slab * slab_cells + receivers).astype(jnp.int32)

    def one_frequency(member):
        frequency, source, observed_now, weight = member
        coupling = frequency * conductivity
        electric = krylov_solve(source, coupling)
        flat_field = electric.reshape(2, 2, 3, NZ * NY * NX)
        misfit = flat_field[..., flat_index] - observed_now
        weight_sq = weight * weight
        adjoint_data = jnp.stack([weight_sq * misfit[:, 0], -weight_sq * misfit[:, 1]], axis=1)
        adjoint_source = jnp.zeros_like(flat_field).at[..., flat_index].add(adjoint_data).reshape(electric.shape)
        adjoint = krylov_solve(adjoint_source, coupling)
        return coupling * lax.optimization_barrier(jnp.sum(adjoint[:, 0] * electric[:, 1] + adjoint[:, 1] * electric[:, 0], axis=(0, 1)))
    freq_terms = lax.map(one_frequency, (omega, sources, observed, data_weight))
    gradient = lax.optimization_barrier(jnp.sum(freq_terms, axis=0))
    mean_square = jnp.mean(gradient * gradient)
    scaled_grad = gradient / jnp.sqrt(mean_square + epsilon)
    beta_ratio = (jnp.sum(scaled_grad * scaled_grad) - jnp.sum(scaled_grad * prior_gradient)) / (jnp.sum(prior_gradient * prior_gradient) + epsilon)
    direction = -scaled_grad + beta_ratio * prior_direction
    unit_direction = direction / jnp.sqrt(jnp.mean(direction * direction) + epsilon)
    trial_model = log_conductivity + step_length[0] * unit_direction
    return (unit_direction, trial_model)
```

```python
import functools

import jax
import jax.numpy as jnp
from jax import lax
from jax.experimental import pallas as pl
from jax.experimental.pallas import tpu as pltpu
from jax.sharding import PartitionSpec as P

ITERS = 4
PAD = 8
EPSILON = 1e-06
POLS = 2

F32 = jnp.float32


def complex_div(dividend, divisor):
    modulus = divisor[0] * divisor[0] + divisor[1] * divisor[1]
    return (
        (dividend[0] * divisor[0] + dividend[1] * divisor[1]) / modulus,
        (dividend[1] * divisor[0] - dividend[0] * divisor[1]) / modulus,
    )


def whole_sum(part):
    return jnp.sum(jnp.sum(part, axis=0, keepdims=True), axis=1, keepdims=True)


def fold(plane):
    return jnp.sum(plane.reshape(-1, 8, plane.shape[-1]), axis=0)


def three_parts(value):
    high = value.astype(jnp.bfloat16)
    rest = value - high.astype(F32)
    middle = rest.astype(jnp.bfloat16)
    low = (rest - middle.astype(F32)).astype(jnp.bfloat16)
    return high, middle, low


def selected(chooser, value):
    total = None
    for part in three_parts(value):
        product = jnp.dot(chooser, part, preferred_element_type=F32)
        total = product if total is None else total + product
    return total


def kernel(
    sizes,
    omega, step_length, sources, log_cond, receivers, observed, weights, prior_grad, prior_dir,
    unit_out, trial_out,
    residual, direction, image, field, adjoint, coupling, log_all, rec_all, obs_all, wgt_all,
    small, term, term_in, flat, outgoing, incoming, own_part, gathered, grad, pg_parts, pd_parts,
    pg_whole, pd_whole, sums_own, sums_in, unit_whole,
    local_sem, slab_send, slab_recv, freq_send, freq_recv, pair_send, pair_recv,
):
    n_freq, n_slab, comps, cz, ny, nx = sizes
    nz, rows = cz * n_slab, cz * ny
    share = rows // n_freq
    own_rows = ny // n_freq
    f, s = lax.axis_index("freq"), lax.axis_index("slab")
    pol = lax.rem(s, POLS)

    own_layers = pl.ds(s * cz, cz)
    local = [
        pltpu.make_async_copy(a, b, local_sem.at[i])
        for i, (a, b) in enumerate(
            [
                (sources.at[0, pol], residual.at[:, :, own_layers]),
                (log_cond, log_all.at[s]),
                (receivers, rec_all.at[s]),
                (observed.at[0, pol], obs_all.at[s]),
                (weights.at[0, pol], wgt_all.at[s]),
                (prior_grad, pg_parts.at[f]),
                (prior_dir, pd_parts.at[f]),
            ]
        )
    ]
    for copy in local:
        copy.start()

    barrier = pltpu.get_barrier_semaphore()

    def greet_slab(j, carry):
        pl.semaphore_signal(barrier, inc=1, device_id={"slab": lax.rem(s + j, n_slab)}, device_id_type=pl.DeviceIdType.MESH)
        return carry

    def greet_freq(k, carry):
        pl.semaphore_signal(barrier, inc=1, device_id={"freq": lax.rem(f + k, n_freq)}, device_id_type=pl.DeviceIdType.MESH)
        return carry

    lax.fori_loop(1, n_freq, greet_freq, 0)
    lax.fori_loop(1, n_slab, greet_slab, 0)

    def to_slab(i, j, source, target):
        return pltpu.make_async_remote_copy(
            src_ref=source, dst_ref=target,
            send_sem=slab_send.at[i, j], recv_sem=slab_recv.at[i, j],
            device_id={"slab": lax.rem(s + j, n_slab)}, device_id_type=pl.DeviceIdType.MESH,
        )

    def to_freq(i, k, source, target):
        return pltpu.make_async_remote_copy(
            src_ref=source, dst_ref=target,
            send_sem=freq_send.at[i, k], recv_sem=freq_recv.at[i, k],
            device_id={"freq": lax.rem(f + k, n_freq)}, device_id_type=pl.DeviceIdType.MESH,
        )

    def slab_inputs(j):
        theirs = lax.rem(lax.rem(s + j, n_slab), POLS)
        return [
            to_slab(0, j, sources.at[0, theirs], residual.at[:, :, own_layers]),
            to_slab(1, j, log_cond, log_all.at[s]),
            to_slab(2, j, receivers, rec_all.at[s]),
            to_slab(3, j, observed.at[0, theirs], obs_all.at[s]),
            to_slab(4, j, weights.at[0, theirs], wgt_all.at[s]),
        ]

    def freq_inputs(k):
        return [
            to_freq(0, k, prior_grad, pg_parts.at[f]),
            to_freq(1, k, prior_dir, pd_parts.at[f]),
        ]

    zero_plane = jnp.zeros((ny + 2 * PAD, nx), F32)
    zero_rows = jnp.zeros((PAD, nx), F32)
    for c in range(2 * comps):
        direction[c, 0] = zero_plane
        direction[c, nz + 1] = zero_plane

    def clear(z, carry):
        for c in range(2 * comps):
            direction[c, z, 0:PAD] = zero_rows
            direction[c, z, PAD + ny:] = zero_rows
        return carry

    lax.fori_loop(1, nz + 1, clear, 0)

    pl.semaphore_wait(barrier, n_freq - 1 + n_slab - 1)
    for j in range(1, n_slab):
        for copy in slab_inputs(j):
            copy.start()

    def start_freq(k, carry):
        for copy in freq_inputs(k):
            copy.start()
        return carry

    lax.fori_loop(1, n_freq, start_freq, 0)
    for copy in local:
        copy.wait()
    for j in range(1, n_slab):
        for copy in slab_inputs(j):
            copy.wait()

    def couple(t, carry):
        coupling[pl.ds(t * cz, cz)] = omega[0] * jnp.exp(log_all[t])
        return carry

    lax.fori_loop(0, n_slab, couple, 0)

    lane = lax.broadcasted_iota(jnp.int32, (ny, nx), 1)
    first, last = lane == 0, lane == nx - 1
    inner = slice(PAD, PAD + ny)
    zero_acc = jnp.zeros((8, nx), F32)

    def product_sum(acc, u, v):
        return (
            acc[0] + fold(u[0] * v[0] - u[1] * v[1]),
            acc[1] + fold(u[0] * v[1] + u[1] * v[0]),
        )

    def totals(acc):
        return whole_sum(acc[0]), whole_sum(acc[1])

    def krylov_solve(target, final):
        def begin(z, acc):
            for c in range(comps):
                b = (residual[0, c, z], residual[1, c, z])
                direction[c, z + 1, inner] = b[0]
                direction[comps + c, z + 1, inner] = b[1]
                acc = product_sum(acc, b, b)
            return acc

        rho = totals(lax.fori_loop(0, nz, begin, (zero_acc, zero_acc)))

        def operate(z, acc):
            coup = coupling[z]
            for c in range(comps):
                laplace, centre = [], []
                for r in range(2):
                    i = r * comps + c
                    d = direction[i, z + 1, inner]
                    beside = direction[i, z + 2, inner] + direction[i, z, inner]
                    beside = beside + direction[i, z + 1, PAD + 1:PAD + 1 + ny]
                    beside = beside + direction[i, z + 1, PAD - 1:PAD - 1 + ny]
                    beside = beside + jnp.where(first, 0.0, pltpu.roll(d, 1, 1))
                    beside = beside + jnp.where(last, 0.0, pltpu.roll(d, nx - 1, 1))
                    laplace.append(6.0 * d - beside)
                    centre.append(d)
                out = (laplace[0] - coup * centre[1], laplace[1] + coup * centre[0])
                image[0, c, z] = out[0]
                image[1, c, z] = out[1]
                acc = product_sum(acc, centre, out)
            return acc

        for iteration in range(ITERS):
            curvature = totals(lax.fori_loop(0, nz, operate, (zero_acc, zero_acc)))
            alpha = complex_div(rho, curvature)
            alpha = (jnp.broadcast_to(alpha[0], (ny, nx)), jnp.broadcast_to(alpha[1], (ny, nx)))
            if iteration + 1 == ITERS:
                lax.fori_loop(0, nz, functools.partial(final, alpha), 0)
                break

            def update(z, acc, alpha=alpha, iteration=iteration):
                for c in range(comps):
                    d = (direction[c, z + 1, inner], direction[comps + c, z + 1, inner])
                    m = (image[0, c, z], image[1, c, z])
                    gain = (alpha[0] * d[0] - alpha[1] * d[1], alpha[0] * d[1] + alpha[1] * d[0])
                    if iteration:
                        gain = (target[0, c, z] + gain[0], target[1, c, z] + gain[1])
                    target[0, c, z] = gain[0]
                    target[1, c, z] = gain[1]
                    left = (
                        residual[0, c, z] - (alpha[0] * m[0] - alpha[1] * m[1]),
                        residual[1, c, z] - (alpha[0] * m[1] + alpha[1] * m[0]),
                    )
                    residual[0, c, z] = left[0]
                    residual[1, c, z] = left[1]
                    acc = product_sum(acc, left, left)
                return acc

            rho_next = totals(lax.fori_loop(0, nz, update, (zero_acc, zero_acc)))
            beta = complex_div(rho_next, rho)
            beta = (jnp.broadcast_to(beta[0], (ny, nx)), jnp.broadcast_to(beta[1], (ny, nx)))
            rho = rho_next

            def turn(z, carry, beta=beta):
                for c in range(comps):
                    d = (direction[c, z + 1, inner], direction[comps + c, z + 1, inner])
                    direction[c, z + 1, inner] = residual[0, c, z] + (beta[0] * d[0] - beta[1] * d[1])
                    direction[comps + c, z + 1, inner] = residual[1, c, z] + (beta[0] * d[1] + beta[1] * d[0])
                return carry

            lax.fori_loop(0, nz, turn, 0)

    def stepped(target, alpha, z, c):
        d = (direction[c, z + 1, inner], direction[comps + c, z + 1, inner])
        return (
            target[0, c, z] + (alpha[0] * d[0] - alpha[1] * d[1]),
            target[1, c, z] + (alpha[0] * d[1] + alpha[1] * d[0]),
        )

    def keep_field(alpha, z, carry):
        for c in range(comps):
            value = stepped(field, alpha, z, c)
            field[0, c, z] = value[0]
            field[1, c, z] = value[1]
        return carry

    krylov_solve(field, keep_field)

    recs = rec_all.shape[-1]
    for t in range(n_slab):
        layers = slice(t * cz, (t + 1) * cz)
        small[0:comps] = obs_all[t, 0]
        small[comps:2 * comps] = obs_all[t, 1]
        small[2 * comps:3 * comps] = wgt_all[t]
        cell = rec_all[t]
        small[3 * comps:3 * comps + 1] = cell.astype(F32)
        columns = small[...].T
        cell_column = columns[:, 3 * comps:3 * comps + 1].astype(jnp.int32)
        row_of = (lax.broadcasted_iota(jnp.int32, (recs, rows), 1) == cell_column // nx)
        lane_of = lax.broadcasted_iota(jnp.int32, (recs, nx), 1) == lax.rem(cell_column, nx)
        row_back = lax.broadcasted_iota(jnp.int32, (rows, recs), 0) == cell // nx
        row_of = row_of.astype(F32).astype(jnp.bfloat16)
        row_back = row_back.astype(F32).astype(jnp.bfloat16)
        values = jnp.concatenate(
            [field[r, c, layers].reshape(rows, nx) for r in range(2) for c in range(comps)], axis=1
        )
        picked = selected(row_of, values)
        spread = []
        for r in range(2):
            for c in range(comps):
                i = r * comps + c
                weight = columns[:, 2 * comps + c:2 * comps + c + 1]
                misfit = picked[:, i * nx:(i + 1) * nx] - columns[:, i:i + 1]
                weight_sq = weight * weight
                spread.append(jnp.where(lane_of, (weight_sq if r == 0 else -weight_sq) * misfit, 0.0))
        back = selected(row_back, jnp.concatenate(spread, axis=1))
        for r in range(2):
            for c in range(comps):
                i = r * comps + c
                residual[r, c, layers] = back[:, i * nx:(i + 1) * nx].reshape(cz, ny, nx)

    def keep_term(alpha, z, carry):
        total = jnp.zeros((ny, nx), F32)
        for c in range(comps):
            value = stepped(adjoint, alpha, z, c)
            total = total + (value[0] * field[1, c, z] + value[1] * field[0, c, z])
        term[z] = coupling[z] * total
        return carry

    krylov_solve(adjoint, keep_term)

    partner = s + 1 - 2 * pol
    swap = pltpu.make_async_remote_copy(
        src_ref=term.at[pl.ds(partner * cz, cz)], dst_ref=term_in,
        send_sem=pair_send, recv_sem=pair_recv,
        device_id={"slab": partner}, device_id_type=pl.DeviceIdType.MESH,
    )
    swap.start()

    def wait_freq(k, carry):
        for copy in freq_inputs(k):
            copy.wait()
        return carry

    lax.fori_loop(1, n_freq, wait_freq, 0)
    swap.wait()

    flat[...] = (term[own_layers] + term_in[...]).reshape(rows, nx)
    for g in range(n_freq):
        outgoing[g] = flat[g * share:(g + 1) * share]

    def scatter(k):
        return to_freq(2, k, outgoing.at[lax.rem(f + k, n_freq)], incoming.at[k])

    def spread_out(k):
        return to_freq(3, k, own_part, gathered.at[f])

    def start_scatter(k, carry):
        scatter(k).start()
        return carry

    lax.fori_loop(1, n_freq, start_scatter, 0)
    for g in range(n_freq):
        pg_whole[:, g * own_rows:(g + 1) * own_rows] = pg_parts[g]
        pd_whole[:, g * own_rows:(g + 1) * own_rows] = pd_parts[g]

    def wait_scatter(k, carry):
        scatter(k).wait()
        return carry

    lax.fori_loop(1, n_freq, wait_scatter, 0)
    mine = outgoing[f]
    for k in range(1, n_freq):
        mine = mine + incoming[k]
    own_part[...] = mine

    def start_spread(k, carry):
        spread_out(k).start()
        return carry

    def wait_spread(k, carry):
        spread_out(k).wait()
        return carry

    lax.fori_loop(1, n_freq, start_spread, 0)
    gathered[f] = mine
    lax.fori_loop(1, n_freq, wait_spread, 0)
    for g in range(n_freq):
        grad[g * share:(g + 1) * share] = gathered[g]

    gradient = grad[...]
    prior = pg_whole[...].reshape(rows, nx)
    before = pd_whole[...].reshape(rows, nx)
    pairs = [(gradient, gradient), (gradient, prior), (prior, prior), (gradient, before), (before, before)]
    for i, (u, v) in enumerate(pairs):
        sums_own[i:i + 1] = jnp.sum(fold(u * v), axis=0, keepdims=True)
    for j in range(1, n_slab):
        to_slab(5, j, sums_own, sums_in.at[j]).start()
    for j in range(1, n_slab):
        to_slab(5, j, sums_own, sums_in.at[j]).wait()
    sums = sums_own[...]
    for j in range(1, n_slab):
        sums = sums + sums_in[j]
    sums = jnp.sum(sums, axis=1, keepdims=True)
    grad_sq, grad_prior, prior_sq, grad_dir, dir_sq = [sums[i:i + 1] for i in range(len(pairs))]
    cells = float(rows * nx * n_slab)
    mean_square = grad_sq / cells
    root_mean = jnp.sqrt(mean_square + EPSILON)
    beta_ratio = (grad_sq / (mean_square + EPSILON) - grad_prior / root_mean) / (prior_sq + EPSILON)
    total = (
        grad_sq / (mean_square + EPSILON)
        - 2.0 * beta_ratio * (grad_dir / root_mean)
        + beta_ratio * beta_ratio * dir_sq
    )
    norm = jnp.sqrt(jnp.maximum(total, 0.0) / cells + EPSILON)
    unit = (gradient * (-1.0 / (root_mean * norm)) + before * (beta_ratio / norm)).reshape(cz, ny, nx)
    trial_out[...] = log_all[s] + step_length[0] * unit
    unit_whole[...] = unit
    unit_out[...] = unit_whole[:, pl.ds(f * own_rows, own_rows), :]


def per_device(n_freq, n_slab, *args):
    (log_cond, omega, sources, receivers, observed, weights, prior_grad, prior_dir, step) = args
    cz, ny, nx = log_cond.shape
    comps = sources.shape[3]
    recs = receivers.shape[0]
    nz, rows = cz * n_slab, cz * ny
    share, own_rows = rows // n_freq, prior_grad.shape[1]
    vec = lambda *shape: pltpu.VMEM(shape, F32)
    dma = lambda *shape: pltpu.SemaphoreType.DMA(shape)
    complex_field = vec(2, comps, nz, ny, nx)
    smem = pl.BlockSpec(memory_space=pltpu.SMEM)
    anywhere = pl.BlockSpec(memory_space=pl.ANY)
    inside = pl.BlockSpec(memory_space=pltpu.VMEM)
    scratch = [
        complex_field,
        vec(2 * comps, nz + 2, ny + 2 * PAD, nx),
        complex_field,
        complex_field,
        complex_field,
        vec(nz, ny, nx),
        vec(n_slab, cz, ny, nx),
        pltpu.VMEM((n_slab, 1, recs), jnp.int32),
        vec(n_slab, 2, comps, recs),
        vec(n_slab, comps, recs),
        vec(16, recs),
        vec(nz, ny, nx),
        vec(cz, ny, nx),
        vec(rows, nx),
        vec(n_freq, share, nx),
        vec(n_freq, share, nx),
        vec(share, nx),
        vec(n_freq, share, nx),
        vec(rows, nx),
        vec(n_freq, cz, own_rows, nx),
        vec(n_freq, cz, own_rows, nx),
        vec(cz, ny, nx),
        vec(cz, ny, nx),
        vec(8, nx),
        vec(n_slab, 8, nx),
        vec(cz, ny, nx),
        dma(7),
        dma(6, n_slab),
        dma(6, n_slab),
        dma(4, n_freq),
        dma(4, n_freq),
        pltpu.SemaphoreType.DMA,
        pltpu.SemaphoreType.DMA,
    ]
    return pl.pallas_call(
        functools.partial(kernel, (n_freq, n_slab, comps, cz, ny, nx)),
        out_shape=(
            jax.ShapeDtypeStruct(prior_grad.shape, F32),
            jax.ShapeDtypeStruct(log_cond.shape, F32),
        ),
        in_specs=[smem, smem] + [anywhere] * 7,
        out_specs=(inside, inside),
        scratch_shapes=scratch,
        compiler_params=pltpu.CompilerParams(
            collective_id=0, has_side_effects=True, vmem_limit_bytes=56 * 1024 * 1024
        ),
        name="inversion",
    )(omega, step, sources, log_cond, receivers.reshape(1, recs), observed, weights, prior_grad, prior_dir)


def solution(mesh):
    in_specs = (
        P("slab", None, None),
        P("freq"),
        P("freq", None, None, None, "slab", None, None),
        P("slab"),
        P("freq", None, None, None, "slab"),
        P("freq", None, None, "slab"),
        P("slab", "freq", None),
        P("slab", "freq", None),
        P(),
    )
    out_specs = (P("slab", "freq", None), P("slab", None, None))
    body = functools.partial(per_device, mesh.shape["freq"], mesh.shape["slab"])
    return jax.shard_map(body, mesh=mesh, in_specs=in_specs, out_specs=out_specs, check_vma=False)
```

```python
import functools

import jax
import jax.numpy as jnp
from jax import lax
from jax.experimental import pallas as pl
from jax.experimental.pallas import tpu as pltpu
from jax.sharding import PartitionSpec as P

ITERS = 4
PAD = 8
EPSILON = 1e-06
POLS = 2

F32 = jnp.float32


def complex_div(dividend, divisor):
    modulus = divisor[0] * divisor[0] + divisor[1] * divisor[1]
    return (
        (dividend[0] * divisor[0] + dividend[1] * divisor[1]) / modulus,
        (dividend[1] * divisor[0] - dividend[0] * divisor[1]) / modulus,
    )


def whole_sum(part):
    return jnp.sum(jnp.sum(part, axis=0, keepdims=True), axis=1, keepdims=True)


def fold(plane):
    return jnp.sum(plane.reshape(-1, 8, plane.shape[-1]), axis=0)


def two_parts(value):
    high = value.astype(jnp.bfloat16)
    return high, (value - high.astype(F32)).astype(jnp.bfloat16)


def selected(chooser, value):
    total = None
    for part in two_parts(value):
        product = jnp.dot(chooser, part, preferred_element_type=F32)
        total = product if total is None else total + product
    return total


def kernel(
    sizes,
    omega, step_length, sources, log_cond, receivers, observed, weights, prior_grad, prior_dir,
    unit_out, trial_out,
    residual, direction, image, field, adjoint, coupling, log_all, rec_all, obs_all, wgt_all,
    small, term, term_in, flat, outgoing, incoming, own_part, gathered, grad, pg_parts, pd_parts,
    pg_whole, pd_whole, sums_own, sums_in, unit_whole,
    local_sem, slab_send, slab_recv, freq_send, freq_recv, pair_send, pair_recv,
):
    n_freq, n_slab, comps, cz, ny, nx = sizes
    nz, rows = cz * n_slab, cz * ny
    share = rows // n_freq
    own_rows = ny // n_freq
    f, s = lax.axis_index("freq"), lax.axis_index("slab")
    pol = lax.rem(s, POLS)

    own_layers = pl.ds(s * cz, cz)
    local = [
        pltpu.make_async_copy(a, b, local_sem.at[i])
        for i, (a, b) in enumerate(
            [
                (sources.at[0, pol], residual.at[:, :, own_layers]),
                (log_cond, log_all.at[s]),
                (receivers, rec_all.at[s]),
                (observed.at[0, pol], obs_all.at[s]),
                (weights.at[0], wgt_all.at[s]),
                (prior_grad, pg_parts.at[f]),
                (prior_dir, pd_parts.at[f]),
            ]
        )
    ]
    for copy in local:
        copy.start()

    barrier = pltpu.get_barrier_semaphore()

    def greet_slab(j, carry):
        pl.semaphore_signal(barrier, inc=1, device_id={"slab": lax.rem(s + j, n_slab)}, device_id_type=pl.DeviceIdType.MESH)
        return carry

    def greet_freq(k, carry):
        pl.semaphore_signal(barrier, inc=1, device_id={"freq": lax.rem(f + k, n_freq)}, device_id_type=pl.DeviceIdType.MESH)
        return carry

    lax.fori_loop(1, n_freq, greet_freq, 0)
    lax.fori_loop(1, n_slab, greet_slab, 0)

    def to_slab(i, j, source, target):
        return pltpu.make_async_remote_copy(
            src_ref=source, dst_ref=target,
            send_sem=slab_send.at[i, j], recv_sem=slab_recv.at[i, j],
            device_id={"slab": lax.rem(s + j, n_slab)}, device_id_type=pl.DeviceIdType.MESH,
        )

    def to_freq(i, k, source, target):
        return pltpu.make_async_remote_copy(
            src_ref=source, dst_ref=target,
            send_sem=freq_send.at[i, k], recv_sem=freq_recv.at[i, k],
            device_id={"freq": lax.rem(f + k, n_freq)}, device_id_type=pl.DeviceIdType.MESH,
        )

    def slab_inputs(j):
        theirs = lax.rem(lax.rem(s + j, n_slab), POLS)
        return [
            to_slab(0, j, sources.at[0, theirs], residual.at[:, :, own_layers]),
            to_slab(1, j, log_cond, log_all.at[s]),
            to_slab(2, j, receivers, rec_all.at[s]),
            to_slab(3, j, observed.at[0, theirs], obs_all.at[s]),
            to_slab(4, j, weights.at[0], wgt_all.at[s]),
        ]

    def freq_inputs(k):
        return [
            to_freq(0, k, prior_grad, pg_parts.at[f]),
            to_freq(1, k, prior_dir, pd_parts.at[f]),
        ]

    zero_plane = jnp.zeros((ny + 2 * PAD, nx), F32)
    zero_rows = jnp.zeros((PAD, nx), F32)
    for c in range(2 * comps):
        direction[c, 0] = zero_plane
        direction[c, nz + 1] = zero_plane

    def clear(z, carry):
        for c in range(2 * comps):
            direction[c, z, 0:PAD] = zero_rows
            direction[c, z, PAD + ny:] = zero_rows
        return carry

    lax.fori_loop(1, nz + 1, clear, 0)

    pl.semaphore_wait(barrier, n_freq - 1 + n_slab - 1)
    for j in range(1, n_slab):
        for copy in slab_inputs(j):
            copy.start()

    def start_freq(k, carry):
        for copy in freq_inputs(k):
            copy.start()
        return carry

    lax.fori_loop(1, n_freq, start_freq, 0)
    for copy in local:
        copy.wait()
    for j in range(1, n_slab):
        for copy in slab_inputs(j):
            copy.wait()

    def couple(t, carry):
        coupling[pl.ds(t * cz, cz)] = omega[0] * jnp.exp(log_all[t])
        return carry

    lax.fori_loop(0, n_slab, couple, 0)

    lane = lax.broadcasted_iota(jnp.int32, (ny, nx), 1)
    first, last = lane == 0, lane == nx - 1
    inner = slice(PAD, PAD + ny)
    zero_acc = jnp.zeros((8, nx), F32)

    def product_sum(acc, u, v):
        return (
            acc[0] + fold(u[0] * v[0] - u[1] * v[1]),
            acc[1] + fold(u[0] * v[1] + u[1] * v[0]),
        )

    def square_sum(acc, u):
        return acc[0] + fold(u[0] * u[0] - u[1] * u[1]), acc[1] + fold(u[0] * u[1])

    def square_totals(acc):
        return whole_sum(acc[0]), 2.0 * whole_sum(acc[1])

    def totals(acc):
        return whole_sum(acc[0]), whole_sum(acc[1])

    def krylov_solve(target, final):
        def begin(z, acc):
            for c in range(comps):
                b = (residual[0, c, z], residual[1, c, z])
                direction[c, z + 1, inner] = b[0]
                direction[comps + c, z + 1, inner] = b[1]
                acc = square_sum(acc, b)
            return acc

        rho = square_totals(lax.fori_loop(0, nz, begin, (zero_acc, zero_acc), unroll=cz))

        def operate(z, acc):
            coup = coupling[z]
            for c in range(comps):
                laplace, centre = [], []
                for r in range(2):
                    i = r * comps + c
                    d = direction[i, z + 1, inner]
                    beside = direction[i, z + 2, inner] + direction[i, z, inner]
                    beside = beside + direction[i, z + 1, PAD + 1:PAD + 1 + ny]
                    beside = beside + direction[i, z + 1, PAD - 1:PAD - 1 + ny]
                    beside = beside + jnp.where(first, 0.0, pltpu.roll(d, 1, 1))
                    beside = beside + jnp.where(last, 0.0, pltpu.roll(d, nx - 1, 1))
                    laplace.append(6.0 * d - beside)
                    centre.append(d)
                out = (laplace[0] - coup * centre[1], laplace[1] + coup * centre[0])
                image[0, c, z] = out[0]
                image[1, c, z] = out[1]
                acc = product_sum(acc, centre, out)
            return acc

        for iteration in range(ITERS):
            curvature = totals(lax.fori_loop(0, nz, operate, (zero_acc, zero_acc), unroll=cz))
            alpha = complex_div(rho, curvature)
            alpha = (jnp.broadcast_to(alpha[0], (ny, nx)), jnp.broadcast_to(alpha[1], (ny, nx)))
            if iteration + 1 == ITERS:
                lax.fori_loop(0, nz, functools.partial(final, alpha), 0, unroll=cz)
                break

            def update(z, acc, alpha=alpha, iteration=iteration):
                for c in range(comps):
                    d = (direction[c, z + 1, inner], direction[comps + c, z + 1, inner])
                    m = (image[0, c, z], image[1, c, z])
                    gain = (alpha[0] * d[0] - alpha[1] * d[1], alpha[0] * d[1] + alpha[1] * d[0])
                    if iteration:
                        gain = (target[0, c, z] + gain[0], target[1, c, z] + gain[1])
                    target[0, c, z] = gain[0]
                    target[1, c, z] = gain[1]
                    left = (
                        residual[0, c, z] - (alpha[0] * m[0] - alpha[1] * m[1]),
                        residual[1, c, z] - (alpha[0] * m[1] + alpha[1] * m[0]),
                    )
                    residual[0, c, z] = left[0]
                    residual[1, c, z] = left[1]
                    acc = square_sum(acc, left)
                return acc

            rho_next = square_totals(lax.fori_loop(0, nz, update, (zero_acc, zero_acc), unroll=cz))
            beta = complex_div(rho_next, rho)
            beta = (jnp.broadcast_to(beta[0], (ny, nx)), jnp.broadcast_to(beta[1], (ny, nx)))
            rho = rho_next

            def turn(z, carry, beta=beta):
                for c in range(comps):
                    d = (direction[c, z + 1, inner], direction[comps + c, z + 1, inner])
                    direction[c, z + 1, inner] = residual[0, c, z] + (beta[0] * d[0] - beta[1] * d[1])
                    direction[comps + c, z + 1, inner] = residual[1, c, z] + (beta[0] * d[1] + beta[1] * d[0])
                return carry

            lax.fori_loop(0, nz, turn, 0, unroll=cz)

    def stepped(target, alpha, z, c):
        d = (direction[c, z + 1, inner], direction[comps + c, z + 1, inner])
        return (
            target[0, c, z] + (alpha[0] * d[0] - alpha[1] * d[1]),
            target[1, c, z] + (alpha[0] * d[1] + alpha[1] * d[0]),
        )

    def keep_field(alpha, z, carry):
        for c in range(comps):
            value = stepped(field, alpha, z, c)
            field[0, c, z] = value[0]
            field[1, c, z] = value[1]
        return carry

    krylov_solve(field, keep_field)

    recs = rec_all.shape[-1]
    for t in range(n_slab):
        layers = slice(t * cz, (t + 1) * cz)
        for c in range(comps):
            small[c:c + 1] = obs_all[t, c, 0:1]
            small[comps + c:comps + c + 1] = obs_all[t, c, 1:2]
            pair = wgt_all[t, c]
            small[2 * comps + c:2 * comps + c + 1] = jnp.where(pol == 0, pair[0:1], pair[1:2])
        cell = rec_all[t]
        small[3 * comps:3 * comps + 1] = cell.astype(F32)
        columns = small[...].T
        cell_column = columns[:, 3 * comps:3 * comps + 1].astype(jnp.int32)
        row_of = (lax.broadcasted_iota(jnp.int32, (recs, rows), 1) == cell_column // nx)
        lane_of = lax.broadcasted_iota(jnp.int32, (recs, nx), 1) == lax.rem(cell_column, nx)
        row_back = lax.broadcasted_iota(jnp.int32, (rows, recs), 0) == cell // nx
        row_of = row_of.astype(F32).astype(jnp.bfloat16)
        row_back = row_back.astype(F32).astype(jnp.bfloat16)
        values = jnp.concatenate(
            [field[r, c, layers].reshape(rows, nx) for r in range(2) for c in range(comps)], axis=1
        )
        picked = selected(row_of, values)
        spread = []
        for r in range(2):
            for c in range(comps):
                i = r * comps + c
                weight = columns[:, 2 * comps + c:2 * comps + c + 1]
                misfit = picked[:, i * nx:(i + 1) * nx] - columns[:, i:i + 1]
                weight_sq = weight * weight
                spread.append(jnp.where(lane_of, (weight_sq if r == 0 else -weight_sq) * misfit, 0.0))
        back = selected(row_back, jnp.concatenate(spread, axis=1))
        for r in range(2):
            for c in range(comps):
                i = r * comps + c
                residual[r, c, layers] = back[:, i * nx:(i + 1) * nx].reshape(cz, ny, nx)

    def keep_term(alpha, z, carry):
        total = jnp.zeros((ny, nx), F32)
        for c in range(comps):
            value = stepped(adjoint, alpha, z, c)
            total = total + (value[0] * field[1, c, z] + value[1] * field[0, c, z])
        term[z] = coupling[z] * total
        return carry

    krylov_solve(adjoint, keep_term)

    partner = s + 1 - 2 * pol
    swap = pltpu.make_async_remote_copy(
        src_ref=term.at[pl.ds(partner * cz, cz)], dst_ref=term_in,
        send_sem=pair_send, recv_sem=pair_recv,
        device_id={"slab": partner}, device_id_type=pl.DeviceIdType.MESH,
    )
    swap.start()

    def wait_freq(k, carry):
        for copy in freq_inputs(k):
            copy.wait()
        return carry

    lax.fori_loop(1, n_freq, wait_freq, 0)
    swap.wait()

    flat[...] = (term[own_layers] + term_in[...]).reshape(rows, nx)
    for g in range(n_freq):
        outgoing[g] = flat[g * share:(g + 1) * share]

    def scatter(k):
        return to_freq(2, k, outgoing.at[lax.rem(f + k, n_freq)], incoming.at[k])

    def spread_out(k):
        return to_freq(3, k, own_part, gathered.at[f])

    def start_scatter(k, carry):
        scatter(k).start()
        return carry

    lax.fori_loop(1, n_freq, start_scatter, 0)
    for g in range(n_freq):
        pg_whole[:, g * own_rows:(g + 1) * own_rows] = pg_parts[g]
        pd_whole[:, g * own_rows:(g + 1) * own_rows] = pd_parts[g]

    def wait_scatter(k, carry):
        scatter(k).wait()
        return carry

    lax.fori_loop(1, n_freq, wait_scatter, 0)
    mine = outgoing[f]
    for k in range(1, n_freq):
        mine = mine + incoming[k]
    own_part[...] = mine

    def start_spread(k, carry):
        spread_out(k).start()
        return carry

    def wait_spread(k, carry):
        spread_out(k).wait()
        return carry

    lax.fori_loop(1, n_freq, start_spread, 0)
    gathered[f] = mine
    lax.fori_loop(1, n_freq, wait_spread, 0)
    for g in range(n_freq):
        grad[g * share:(g + 1) * share] = gathered[g]

    gradient = grad[...]
    prior = pg_whole[...].reshape(rows, nx)
    before = pd_whole[...].reshape(rows, nx)
    pairs = [(gradient, gradient), (gradient, prior), (prior, prior), (gradient, before), (before, before)]
    for i, (u, v) in enumerate(pairs):
        sums_own[i:i + 1] = jnp.sum(fold(u * v), axis=0, keepdims=True)
    for j in range(1, n_slab):
        to_slab(5, j, sums_own, sums_in.at[j]).start()
    for j in range(1, n_slab):
        to_slab(5, j, sums_own, sums_in.at[j]).wait()
    sums = sums_own[...]
    for j in range(1, n_slab):
        sums = sums + sums_in[j]
    sums = jnp.sum(sums, axis=1, keepdims=True)
    grad_sq, grad_prior, prior_sq, grad_dir, dir_sq = [sums[i:i + 1] for i in range(len(pairs))]
    cells = float(rows * nx * n_slab)
    mean_square = grad_sq / cells
    root_mean = jnp.sqrt(mean_square + EPSILON)
    beta_ratio = (grad_sq / (mean_square + EPSILON) - grad_prior / root_mean) / (prior_sq + EPSILON)
    total = (
        grad_sq / (mean_square + EPSILON)
        - 2.0 * beta_ratio * (grad_dir / root_mean)
        + beta_ratio * beta_ratio * dir_sq
    )
    norm = jnp.sqrt(jnp.maximum(total, 0.0) / cells + EPSILON)
    unit = (gradient * (-1.0 / (root_mean * norm)) + before * (beta_ratio / norm)).reshape(cz, ny, nx)
    trial_out[...] = log_all[s] + step_length[0] * unit
    unit_whole[...] = unit
    unit_out[...] = unit_whole[:, pl.ds(f * own_rows, own_rows), :]


def per_device(n_freq, n_slab, *args):
    (log_cond, omega, sources, receivers, observed, weights, prior_grad, prior_dir, step) = args
    cz, ny, nx = log_cond.shape
    comps = sources.shape[3]
    recs = receivers.shape[0]
    nz, rows = cz * n_slab, cz * ny
    share, own_rows = rows // n_freq, prior_grad.shape[1]
    vec = lambda *shape: pltpu.VMEM(shape, F32)
    dma = lambda *shape: pltpu.SemaphoreType.DMA(shape)
    complex_field = vec(2, comps, nz, ny, nx)
    smem = pl.BlockSpec(memory_space=pltpu.SMEM)
    anywhere = pl.BlockSpec(memory_space=pl.ANY)
    inside = pl.BlockSpec(memory_space=pltpu.VMEM)
    scratch = [
        complex_field,
        vec(2 * comps, nz + 2, ny + 2 * PAD, nx),
        complex_field,
        complex_field,
        complex_field,
        vec(nz, ny, nx),
        vec(n_slab, cz, ny, nx),
        pltpu.VMEM((n_slab, 1, recs), jnp.int32),
        vec(n_slab, comps, 2, recs),
        vec(n_slab, comps, POLS, recs),
        vec(16, recs),
        vec(nz, ny, nx),
        vec(cz, ny, nx),
        vec(rows, nx),
        vec(n_freq, share, nx),
        vec(n_freq, share, nx),
        vec(share, nx),
        vec(n_freq, share, nx),
        vec(rows, nx),
        vec(n_freq, cz, own_rows, nx),
        vec(n_freq, cz, own_rows, nx),
        vec(cz, ny, nx),
        vec(cz, ny, nx),
        vec(8, nx),
        vec(n_slab, 8, nx),
        vec(cz, ny, nx),
        dma(7),
        dma(6, n_slab),
        dma(6, n_slab),
        dma(4, n_freq),
        dma(4, n_freq),
        pltpu.SemaphoreType.DMA,
        pltpu.SemaphoreType.DMA,
    ]
    unit, trial = pl.pallas_call(
        functools.partial(kernel, (n_freq, n_slab, comps, cz, ny, nx)),
        out_shape=(
            jax.ShapeDtypeStruct(prior_grad.shape, F32),
            jax.ShapeDtypeStruct(log_cond.shape, F32),
        ),
        in_specs=[smem, smem] + [anywhere] * 7,
        out_specs=(inside, inside),
        scratch_shapes=scratch,
        compiler_params=pltpu.CompilerParams(
            collective_id=0, has_side_effects=True, vmem_limit_bytes=56 * 1024 * 1024
        ),
        name="inversion",
    )(omega, step, sources, log_cond, receivers.reshape(1, recs), jnp.swapaxes(observed, 2, 3),
      jnp.swapaxes(weights, 1, 2), prior_grad, prior_dir)
    return pl.pallas_call(
        hand_over,
        out_shape=(
            jax.ShapeDtypeStruct(unit.shape, F32),
            jax.ShapeDtypeStruct(trial.shape, F32),
        ),
        in_specs=[inside, inside],
        out_specs=(inside, inside),
        name="hand_over",
    )(unit, trial)


def hand_over(unit, trial, unit_out, trial_out):
    unit_out[...] = unit[...]
    trial_out[...] = trial[...]


def solution(mesh):
    in_specs = (
        P("slab", None, None),
        P("freq"),
        P("freq", None, None, None, "slab", None, None),
        P("slab"),
        P("freq", None, None, None, "slab"),
        P("freq", None, None, "slab"),
        P("slab", "freq", None),
        P("slab", "freq", None),
        P(),
    )
    out_specs = (P("slab", "freq", None), P("slab", None, None))
    body = functools.partial(per_device, mesh.shape["freq"], mesh.shape["slab"])
    return jax.shard_map(body, mesh=mesh, in_specs=in_specs, out_specs=out_specs, check_vma=False)
```

```python
import functools

import jax
import jax.numpy as jnp
from jax import lax
from jax.experimental import pallas as pl
from jax.experimental.pallas import tpu as pltpu
from jax.sharding import PartitionSpec as P

ITERS = 4
PAD = 8
EPSILON = 1e-06
POLS = 2

F32 = jnp.float32


def complex_div(dividend, divisor):
    modulus = divisor[0] * divisor[0] + divisor[1] * divisor[1]
    return (
        (dividend[0] * divisor[0] + dividend[1] * divisor[1]) / modulus,
        (dividend[1] * divisor[0] - dividend[0] * divisor[1]) / modulus,
    )


def whole_sum(part):
    return jnp.sum(jnp.sum(part, axis=0, keepdims=True), axis=1, keepdims=True)


def fold(plane):
    return jnp.sum(plane.reshape(-1, 8, plane.shape[-1]), axis=0)


def two_parts(value):
    high = value.astype(jnp.bfloat16)
    return high, (value - high.astype(F32)).astype(jnp.bfloat16)


def selected(chooser, value):
    total = None
    for part in two_parts(value):
        product = jnp.dot(chooser, part, preferred_element_type=F32)
        total = product if total is None else total + product
    return total


def exchange(
    n_slab,
    sources, log_cond, receivers, observed, weights,
    sources_in, log_in, rec_in, obs_in, wgt_in,
    send, recv,
):
    s = lax.axis_index("slab")
    barrier = pltpu.get_barrier_semaphore()

    def peer(j):
        return {"slab": lax.rem(s + j, n_slab)}

    for j in range(1, n_slab):
        pl.semaphore_signal(barrier, inc=1, device_id=peer(j), device_id_type=pl.DeviceIdType.MESH)
    pl.semaphore_wait(barrier, n_slab - 1)
    copies = []
    for j in range(1, n_slab):
        theirs = lax.rem(lax.rem(s + j, n_slab), POLS)
        moves = [
            (sources.at[0, theirs], sources_in.at[j - 1]),
            (log_cond, log_in.at[j - 1]),
            (receivers, rec_in.at[j - 1]),
            (observed.at[0, theirs], obs_in.at[j - 1]),
            (weights.at[0], wgt_in.at[j - 1]),
        ]
        for i, (source, target) in enumerate(moves):
            copies.append(
                pltpu.make_async_remote_copy(
                    src_ref=source, dst_ref=target, send_sem=send.at[i, j], recv_sem=recv.at[i, j],
                    device_id=peer(j), device_id_type=pl.DeviceIdType.MESH,
                )
            )
    for copy in copies:
        copy.start()
    for copy in copies:
        copy.wait()


def kernel(
    sizes,
    omega, step_length, sources, log_cond, receivers, observed, weights, prior_grad, prior_dir,
    sources_in, log_in, rec_in, obs_in, wgt_in,
    unit_out, trial_out,
    residual, direction, image, field, adjoint, coupling, log_all, rec_all, obs_all, wgt_all,
    small, term, term_in, flat, outgoing, incoming, own_part, gathered, grad, pg_parts, pd_parts,
    pg_whole, pd_whole, sums_own, sums_in, unit_whole,
    local_sem, near_sem, slab_send, slab_recv, freq_send, freq_recv, pair_send, pair_recv,
):
    n_freq, n_slab, comps, cz, ny, nx = sizes
    nz, rows = cz * n_slab, cz * ny
    share = rows // n_freq
    own_rows = ny // n_freq
    f, s = lax.axis_index("freq"), lax.axis_index("slab")
    pol = lax.rem(s, POLS)

    own_layers = pl.ds(s * cz, cz)
    local = [
        pltpu.make_async_copy(a, b, local_sem.at[i])
        for i, (a, b) in enumerate(
            [
                (sources.at[0, pol], residual.at[:, :, own_layers]),
                (log_cond, log_all.at[s]),
                (receivers, rec_all.at[s]),
                (observed.at[0, pol], obs_all.at[s]),
                (weights.at[0], wgt_all.at[s]),
                (prior_grad, pg_parts.at[f]),
                (prior_dir, pd_parts.at[f]),
            ]
        )
    ]
    for j in range(1, n_slab):
        t = lax.rem(s + n_slab - j, n_slab)
        moves = [
            (sources_in.at[j - 1], residual.at[:, :, pl.ds(t * cz, cz)]),
            (log_in.at[j - 1], log_all.at[t]),
            (rec_in.at[j - 1], rec_all.at[t]),
            (obs_in.at[j - 1], obs_all.at[t]),
            (wgt_in.at[j - 1], wgt_all.at[t]),
        ]
        for i, (a, b) in enumerate(moves):
            local.append(pltpu.make_async_copy(a, b, near_sem.at[i, j]))
    for copy in local:
        copy.start()

    barrier = pltpu.get_barrier_semaphore()

    def greet_slab(j, carry):
        pl.semaphore_signal(barrier, inc=1, device_id={"slab": lax.rem(s + j, n_slab)}, device_id_type=pl.DeviceIdType.MESH)
        return carry

    def greet_freq(k, carry):
        pl.semaphore_signal(barrier, inc=1, device_id={"freq": lax.rem(f + k, n_freq)}, device_id_type=pl.DeviceIdType.MESH)
        return carry

    lax.fori_loop(1, n_freq, greet_freq, 0)
    lax.fori_loop(1, n_slab, greet_slab, 0)

    def to_slab(j, source, target):
        return pltpu.make_async_remote_copy(
            src_ref=source, dst_ref=target,
            send_sem=slab_send.at[j], recv_sem=slab_recv.at[j],
            device_id={"slab": lax.rem(s + j, n_slab)}, device_id_type=pl.DeviceIdType.MESH,
        )

    def to_freq(i, k, source, target):
        return pltpu.make_async_remote_copy(
            src_ref=source, dst_ref=target,
            send_sem=freq_send.at[i, k], recv_sem=freq_recv.at[i, k],
            device_id={"freq": lax.rem(f + k, n_freq)}, device_id_type=pl.DeviceIdType.MESH,
        )

    def freq_inputs(k):
        return [
            to_freq(0, k, prior_grad, pg_parts.at[f]),
            to_freq(1, k, prior_dir, pd_parts.at[f]),
        ]

    zero_plane = jnp.zeros((ny + 2 * PAD, nx), F32)
    zero_rows = jnp.zeros((PAD, nx), F32)
    for c in range(2 * comps):
        direction[c, 0] = zero_plane
        direction[c, nz + 1] = zero_plane

    def clear(z, carry):
        for c in range(2 * comps):
            direction[c, z, 0:PAD] = zero_rows
            direction[c, z, PAD + ny:] = zero_rows
        return carry

    lax.fori_loop(1, nz + 1, clear, 0)

    for copy in local:
        copy.wait()

    def couple(t, carry):
        coupling[pl.ds(t * cz, cz)] = omega[0] * jnp.exp(log_all[t])
        return carry

    lax.fori_loop(0, n_slab, couple, 0)

    lane = lax.broadcasted_iota(jnp.int32, (ny, nx), 1)
    first, last = lane == 0, lane == nx - 1
    inner = slice(PAD, PAD + ny)
    zero_acc = jnp.zeros((8, nx), F32)

    def product_sum(acc, u, v):
        return (
            acc[0] + fold(u[0] * v[0] - u[1] * v[1]),
            acc[1] + fold(u[0] * v[1] + u[1] * v[0]),
        )

    def square_sum(acc, u):
        return acc[0] + fold(u[0] * u[0] - u[1] * u[1]), acc[1] + fold(u[0] * u[1])

    def square_totals(acc):
        return whole_sum(acc[0]), 2.0 * whole_sum(acc[1])

    def totals(acc):
        return whole_sum(acc[0]), whole_sum(acc[1])

    def krylov_solve(target, final):
        def begin(z, acc):
            for c in range(comps):
                b = (residual[0, c, z], residual[1, c, z])
                direction[c, z + 1, inner] = b[0]
                direction[comps + c, z + 1, inner] = b[1]
                acc = square_sum(acc, b)
            return acc

        rho = square_totals(lax.fori_loop(0, nz, begin, (zero_acc, zero_acc), unroll=cz))

        def operate(z, acc):
            coup = coupling[z]
            for c in range(comps):
                laplace, centre = [], []
                for r in range(2):
                    i = r * comps + c
                    d = direction[i, z + 1, inner]
                    beside = direction[i, z + 2, inner] + direction[i, z, inner]
                    beside = beside + direction[i, z + 1, PAD + 1:PAD + 1 + ny]
                    beside = beside + direction[i, z + 1, PAD - 1:PAD - 1 + ny]
                    beside = beside + jnp.where(first, 0.0, pltpu.roll(d, 1, 1))
                    beside = beside + jnp.where(last, 0.0, pltpu.roll(d, nx - 1, 1))
                    laplace.append(6.0 * d - beside)
                    centre.append(d)
                out = (laplace[0] - coup * centre[1], laplace[1] + coup * centre[0])
                image[0, c, z] = out[0]
                image[1, c, z] = out[1]
                acc = product_sum(acc, centre, out)
            return acc

        for iteration in range(ITERS):
            curvature = totals(lax.fori_loop(0, nz, operate, (zero_acc, zero_acc), unroll=cz))
            alpha = complex_div(rho, curvature)
            alpha = (jnp.broadcast_to(alpha[0], (ny, nx)), jnp.broadcast_to(alpha[1], (ny, nx)))
            if iteration + 1 == ITERS:
                lax.fori_loop(0, nz, functools.partial(final, alpha), 0, unroll=cz)
                break

            def update(z, acc, alpha=alpha, iteration=iteration):
                for c in range(comps):
                    d = (direction[c, z + 1, inner], direction[comps + c, z + 1, inner])
                    m = (image[0, c, z], image[1, c, z])
                    gain = (alpha[0] * d[0] - alpha[1] * d[1], alpha[0] * d[1] + alpha[1] * d[0])
                    if iteration:
                        gain = (target[0, c, z] + gain[0], target[1, c, z] + gain[1])
                    target[0, c, z] = gain[0]
                    target[1, c, z] = gain[1]
                    left = (
                        residual[0, c, z] - (alpha[0] * m[0] - alpha[1] * m[1]),
                        residual[1, c, z] - (alpha[0] * m[1] + alpha[1] * m[0]),
                    )
                    residual[0, c, z] = left[0]
                    residual[1, c, z] = left[1]
                    acc = square_sum(acc, left)
                return acc

            rho_next = square_totals(lax.fori_loop(0, nz, update, (zero_acc, zero_acc), unroll=cz))
            beta = complex_div(rho_next, rho)
            beta = (jnp.broadcast_to(beta[0], (ny, nx)), jnp.broadcast_to(beta[1], (ny, nx)))
            rho = rho_next

            def turn(z, carry, beta=beta):
                for c in range(comps):
                    d = (direction[c, z + 1, inner], direction[comps + c, z + 1, inner])
                    direction[c, z + 1, inner] = residual[0, c, z] + (beta[0] * d[0] - beta[1] * d[1])
                    direction[comps + c, z + 1, inner] = residual[1, c, z] + (beta[0] * d[1] + beta[1] * d[0])
                return carry

            lax.fori_loop(0, nz, turn, 0, unroll=cz)

    def stepped(target, alpha, z, c):
        d = (direction[c, z + 1, inner], direction[comps + c, z + 1, inner])
        return (
            target[0, c, z] + (alpha[0] * d[0] - alpha[1] * d[1]),
            target[1, c, z] + (alpha[0] * d[1] + alpha[1] * d[0]),
        )

    def keep_field(alpha, z, carry):
        for c in range(comps):
            value = stepped(field, alpha, z, c)
            field[0, c, z] = value[0]
            field[1, c, z] = value[1]
        return carry

    krylov_solve(field, keep_field)

    pl.semaphore_wait(barrier, n_freq - 1 + n_slab - 1)

    def start_freq(k, carry):
        for copy in freq_inputs(k):
            copy.start()
        return carry

    lax.fori_loop(1, n_freq, start_freq, 0)

    recs = rec_all.shape[-1]
    for t in range(n_slab):
        layers = slice(t * cz, (t + 1) * cz)
        for c in range(comps):
            small[c:c + 1] = obs_all[t, c, 0:1]
            small[comps + c:comps + c + 1] = obs_all[t, c, 1:2]
            pair = wgt_all[t, c]
            small[2 * comps + c:2 * comps + c + 1] = jnp.where(pol == 0, pair[0:1], pair[1:2])
        cell = rec_all[t]
        small[3 * comps:3 * comps + 1] = cell.astype(F32)
        columns = small[...].T
        cell_column = columns[:, 3 * comps:3 * comps + 1].astype(jnp.int32)
        row_of = (lax.broadcasted_iota(jnp.int32, (recs, rows), 1) == cell_column // nx)
        lane_of = lax.broadcasted_iota(jnp.int32, (recs, nx), 1) == lax.rem(cell_column, nx)
        row_back = lax.broadcasted_iota(jnp.int32, (rows, recs), 0) == cell // nx
        row_of = row_of.astype(F32).astype(jnp.bfloat16)
        row_back = row_back.astype(F32).astype(jnp.bfloat16)
        values = jnp.concatenate(
            [field[r, c, layers].reshape(rows, nx) for r in range(2) for c in range(comps)], axis=1
        )
        picked = selected(row_of, values)
        spread = []
        for r in range(2):
            for c in range(comps):
                i = r * comps + c
                weight = columns[:, 2 * comps + c:2 * comps + c + 1]
                misfit = picked[:, i * nx:(i + 1) * nx] - columns[:, i:i + 1]
                weight_sq = weight * weight
                spread.append(jnp.where(lane_of, (weight_sq if r == 0 else -weight_sq) * misfit, 0.0))
        back = selected(row_back, jnp.concatenate(spread, axis=1))
        for r in range(2):
            for c in range(comps):
                i = r * comps + c
                residual[r, c, layers] = back[:, i * nx:(i + 1) * nx].reshape(cz, ny, nx)

    def keep_term(alpha, z, carry):
        total = jnp.zeros((ny, nx), F32)
        for c in range(comps):
            value = stepped(adjoint, alpha, z, c)
            total = total + (value[0] * field[1, c, z] + value[1] * field[0, c, z])
        term[z] = coupling[z] * total
        return carry

    krylov_solve(adjoint, keep_term)

    partner = s + 1 - 2 * pol
    swap = pltpu.make_async_remote_copy(
        src_ref=term.at[pl.ds(partner * cz, cz)], dst_ref=term_in,
        send_sem=pair_send, recv_sem=pair_recv,
        device_id={"slab": partner}, device_id_type=pl.DeviceIdType.MESH,
    )
    swap.start()

    def wait_freq(k, carry):
        for copy in freq_inputs(k):
            copy.wait()
        return carry

    lax.fori_loop(1, n_freq, wait_freq, 0)
    swap.wait()

    flat[...] = (term[own_layers] + term_in[...]).reshape(rows, nx)
    for g in range(n_freq):
        outgoing[g] = flat[g * share:(g + 1) * share]

    def scatter(k):
        return to_freq(2, k, outgoing.at[lax.rem(f + k, n_freq)], incoming.at[k])

    def spread_out(k):
        return to_freq(3, k, own_part, gathered.at[f])

    def start_scatter(k, carry):
        scatter(k).start()
        return carry

    lax.fori_loop(1, n_freq, start_scatter, 0)
    for g in range(n_freq):
        pg_whole[:, g * own_rows:(g + 1) * own_rows] = pg_parts[g]
        pd_whole[:, g * own_rows:(g + 1) * own_rows] = pd_parts[g]

    def wait_scatter(k, carry):
        scatter(k).wait()
        return carry

    lax.fori_loop(1, n_freq, wait_scatter, 0)
    mine = outgoing[f]
    for k in range(1, n_freq):
        mine = mine + incoming[k]
    own_part[...] = mine

    def start_spread(k, carry):
        spread_out(k).start()
        return carry

    def wait_spread(k, carry):
        spread_out(k).wait()
        return carry

    lax.fori_loop(1, n_freq, start_spread, 0)
    gathered[f] = mine
    lax.fori_loop(1, n_freq, wait_spread, 0)
    for g in range(n_freq):
        grad[g * share:(g + 1) * share] = gathered[g]

    gradient = grad[...]
    prior = pg_whole[...].reshape(rows, nx)
    before = pd_whole[...].reshape(rows, nx)
    pairs = [(gradient, gradient), (gradient, prior), (prior, prior), (gradient, before), (before, before)]
    for i, (u, v) in enumerate(pairs):
        sums_own[i:i + 1] = jnp.sum(fold(u * v), axis=0, keepdims=True)
    for j in range(1, n_slab):
        to_slab(j, sums_own, sums_in.at[j]).start()
    for j in range(1, n_slab):
        to_slab(j, sums_own, sums_in.at[j]).wait()
    sums = sums_own[...]
    for j in range(1, n_slab):
        sums = sums + sums_in[j]
    sums = jnp.sum(sums, axis=1, keepdims=True)
    grad_sq, grad_prior, prior_sq, grad_dir, dir_sq = [sums[i:i + 1] for i in range(len(pairs))]
    cells = float(rows * nx * n_slab)
    mean_square = grad_sq / cells
    root_mean = jnp.sqrt(mean_square + EPSILON)
    beta_ratio = (grad_sq / (mean_square + EPSILON) - grad_prior / root_mean) / (prior_sq + EPSILON)
    total = (
        grad_sq / (mean_square + EPSILON)
        - 2.0 * beta_ratio * (grad_dir / root_mean)
        + beta_ratio * beta_ratio * dir_sq
    )
    norm = jnp.sqrt(jnp.maximum(total, 0.0) / cells + EPSILON)
    unit = (gradient * (-1.0 / (root_mean * norm)) + before * (beta_ratio / norm)).reshape(cz, ny, nx)
    trial_out[...] = log_all[s] + step_length[0] * unit
    unit_whole[...] = unit
    unit_out[...] = unit_whole[:, pl.ds(f * own_rows, own_rows), :]


def per_device(n_freq, n_slab, *args):
    (log_cond, omega, sources, receivers, observed, weights, prior_grad, prior_dir, step) = args
    cz, ny, nx = log_cond.shape
    comps = sources.shape[3]
    recs = receivers.shape[0]
    nz, rows = cz * n_slab, cz * ny
    share, own_rows = rows // n_freq, prior_grad.shape[1]
    vec = lambda *shape: pltpu.VMEM(shape, F32)
    dma = lambda *shape: pltpu.SemaphoreType.DMA(shape)
    complex_field = vec(2, comps, nz, ny, nx)
    smem = pl.BlockSpec(memory_space=pltpu.SMEM)
    anywhere = pl.BlockSpec(memory_space=pl.ANY)
    inside = pl.BlockSpec(memory_space=pltpu.VMEM)
    scratch = [
        complex_field,
        vec(2 * comps, nz + 2, ny + 2 * PAD, nx),
        complex_field,
        complex_field,
        complex_field,
        vec(nz, ny, nx),
        vec(n_slab, cz, ny, nx),
        pltpu.VMEM((n_slab, 1, recs), jnp.int32),
        vec(n_slab, comps, 2, recs),
        vec(n_slab, comps, POLS, recs),
        vec(16, recs),
        vec(nz, ny, nx),
        vec(cz, ny, nx),
        vec(rows, nx),
        vec(n_freq, share, nx),
        vec(n_freq, share, nx),
        vec(share, nx),
        vec(n_freq, share, nx),
        vec(rows, nx),
        vec(n_freq, cz, own_rows, nx),
        vec(n_freq, cz, own_rows, nx),
        vec(cz, ny, nx),
        vec(cz, ny, nx),
        vec(8, nx),
        vec(n_slab, 8, nx),
        vec(cz, ny, nx),
        dma(7),
        dma(5, n_slab),
        dma(n_slab),
        dma(n_slab),
        dma(4, n_freq),
        dma(4, n_freq),
        pltpu.SemaphoreType.DMA,
        pltpu.SemaphoreType.DMA,
    ]
    local = (sources, log_cond, receivers.reshape(1, recs), jnp.swapaxes(observed, 2, 3), jnp.swapaxes(weights, 1, 2))
    others = n_slab - 1
    arrived = [(2, comps, cz, ny, nx), (cz, ny, nx), (1, recs), (comps, 2, recs), (comps, POLS, recs)]
    far = pl.pallas_call(
        functools.partial(exchange, n_slab),
        out_shape=[
            jax.ShapeDtypeStruct((others, *shape), value.dtype) for shape, value in zip(arrived, local)
        ],
        in_specs=[anywhere] * 5,
        out_specs=[anywhere] * 5,
        scratch_shapes=[dma(5, n_slab), dma(5, n_slab)],
        compiler_params=pltpu.CompilerParams(collective_id=1, has_side_effects=True),
        name="exchange",
    )(*local)
    unit, trial = pl.pallas_call(
        functools.partial(kernel, (n_freq, n_slab, comps, cz, ny, nx)),
        out_shape=(
            jax.ShapeDtypeStruct(prior_grad.shape, F32),
            jax.ShapeDtypeStruct(log_cond.shape, F32),
        ),
        in_specs=[smem, smem] + [anywhere] * 12,
        out_specs=(inside, inside),
        scratch_shapes=scratch,
        compiler_params=pltpu.CompilerParams(
            collective_id=0, has_side_effects=True, vmem_limit_bytes=56 * 1024 * 1024
        ),
        name="inversion",
    )(omega, step, *local, prior_grad, prior_dir, *far)
    return pl.pallas_call(
        hand_over,
        out_shape=(
            jax.ShapeDtypeStruct(unit.shape, F32),
            jax.ShapeDtypeStruct(trial.shape, F32),
        ),
        in_specs=[inside, inside],
        out_specs=(inside, inside),
        name="hand_over",
    )(unit, trial)


def hand_over(unit, trial, unit_out, trial_out):
    unit_out[...] = unit[...]
    trial_out[...] = trial[...]


def solution(mesh):
    in_specs = (
        P("slab", None, None),
        P("freq"),
        P("freq", None, None, None, "slab", None, None),
        P("slab"),
        P("freq", None, None, None, "slab"),
        P("freq", None, None, "slab"),
        P("slab", "freq", None),
        P("slab", "freq", None),
        P(),
    )
    out_specs = (P("slab", "freq", None), P("slab", None, None))
    body = functools.partial(per_device, mesh.shape["freq"], mesh.shape["slab"])
    return jax.shard_map(body, mesh=mesh, in_specs=in_specs, out_specs=out_specs, check_vma=False)
```
